32 devices in a mesh: rep: 16 (over z, x, core), slab: 2 (over y).
Axes of the slice: x: 2, y: 2, z: 4, core: 2. Of those that a mesh axis runs over, the one named last changes fastest.
Arguments:
- weights: bfloat16 [16, 256, 3072], P('rep', 'slab'), may hold values from -6 to 6
- perms: int32 [16, 8, 256], P('rep'), may hold values from 0 to 255, each once within a row
Outputs:
- merged: bfloat16 [16, 256, 3072], P('rep', 'slab')
The draws below stay inside these ranges and needn't reach their ends.
Inputs may be any that keep to these rules, and one draw needn't show every extreme that they name: `perms`: each row of 256 entries names every neuron of the window once.
All inputs are finite; a program needn't handle non-finite values.
Results may differ from the reference program's by a relative error of at most 0.012.
Values may be sent and summed in bfloat16 or wider, within the bound.
A program may use at most 64 MiB of HBM per device.

```python
import math
import jax
import jax.numpy as jnp
from jax import lax

D = 3072
ROUNDS = 8
FFW = 256
REPLICAS = 16
N_REP = 16


def shard_levels(own_key, dims, cuts, smallest, top_value):
    loudness = 1.0
    for axis_at, parts in cuts:
        heights = jax.random.uniform(jax.random.fold_in(jax.random.fold_in(own_key, 6), axis_at), (parts,), jnp.float32, smallest / len(cuts), top_value / len(cuts))
        loudness = loudness * jnp.repeat(jnp.exp(heights), dims[axis_at] // parts).reshape((-1,) + (1,) * (len(dims) - 1 - axis_at))
    return loudness


def gaussian(own_key, shape, deviation, bound, split=(), kind=jnp.bfloat16):
    array = deviation * jax.random.normal(own_key, shape, jnp.float32)
    if split:
        array = array * shard_levels(own_key, shape, split, -0.22, 0.18)
    return jnp.clip(array, -bound, bound).astype(kind)


def setup_inputs(seed: int = 0) -> dict:
    arg_keys = jax.random.split(jax.random.key(seed), 3)
    weights = gaussian(arg_keys[0], (REPLICAS, FFW, D), 1.0, 6.0, ((0, 16), (1, 2)))
    perms = jax.vmap(lambda own: jax.random.permutation(own, FFW))(jax.random.split(arg_keys[1], REPLICAS * ROUNDS)).reshape((REPLICAS, ROUNDS, FFW)).astype(jnp.int32)
    return dict(weights=weights, perms=perms)


def merge_one(own, partner, perm_row):
    cost = jnp.dot(own, partner.T, preferred_element_type=jnp.float32) * (1.0 / math.sqrt(D))
    squared = cost * cost
    fourth = squared * squared
    soft_plan = fourth / (1.0 + lax.optimization_barrier(jnp.sum(fourth, axis=1, keepdims=True)))
    columns = jnp.arange(partner.shape[0], dtype=jnp.int32)
    onehot = (perm_row[:, None] == columns[None, :]).astype(jnp.float32)
    mixing = (onehot + soft_plan).astype(jnp.bfloat16)
    aligned = 0.5 * jnp.dot(mixing, partner, preferred_element_type=jnp.float32)
    return ((own.astype(jnp.float32) + aligned) * (1.0 / math.sqrt(2.0))).astype(jnp.bfloat16)

def reference(weights, perms):
    bit_count = N_REP.bit_length() - 1
    current = weights
    for round_idx in range(ROUNDS):
        flip = 1 << round_idx % bit_count
        partner_idx = jnp.bitwise_xor(jnp.arange(REPLICAS, dtype=jnp.int32), flip)
        partner = current[partner_idx]
        current = jax.vmap(merge_one)(current, partner, perms[:, round_idx])
    return current
```

```python
import functools
import math

import jax
import jax.numpy as jnp
from jax import lax
from jax.experimental import pallas as pl
from jax.experimental.pallas import tpu as pltpu
from jax.sharding import PartitionSpec as P

CHUNK = 256


def placements(bits, rounds):
    position = {b: b for b in range(1, bits)}
    plan = [(0, None, dict(position))]
    for r in range(1, rounds):
        old, new = (r - 1) % bits, r % bits
        device_bit = position.pop(new)
        position[old] = device_bit
        plan.append((new, device_bit, dict(position)))
    return plan


def kernel(n_rep, n_slab, rounds, w_ref, p_ref, out_ref,
           state, sent, kept, part, core_in, slab_out, slab_in, cost_ref, perms,
           in_send, in_recv, ex_send, ex_recv, core_send, core_recv, slab_send, slab_recv,
           cost_send, cost_recv, out_send, out_recv, perm_send, perm_recv):
    bits = n_rep.bit_length() - 1
    me = lax.axis_index("rep")
    slab = lax.axis_index("slab")
    core = me % 2
    half, width = w_ref.shape[1], w_ref.shape[2]
    ffw = half * n_slab
    block = width // (2 * n_slab)
    chunks = block // CHUNK
    plan = placements(bits, rounds)

    def bit(b):
        return (me // (1 << b)) % 2

    def flipped(b):
        return me + (1 - 2 * bit(b)) * (1 << b)

    def remote(src, dst, send, recv, rep_to, slab_to):
        return pltpu.make_async_remote_copy(
            src_ref=src, dst_ref=dst, send_sem=send, recv_sem=recv,
            device_id=(rep_to, slab_to), device_id_type=pl.DeviceIdType.MESH)

    first_waits = []
    rows_here = pl.ds(pl.multiple_of(slab * half, half), half)
    for k in range(chunks):
        for ds_ in range(n_slab):
            for dc in range(2):
                rep_to = me if dc == 0 else flipped(0)
                core_to = core if dc == 0 else 1 - core
                slab_to = (slab + ds_) % n_slab
                start = (slab_to * 2 + core_to) * block + k * CHUNK
                src = w_ref.at[0, :, pl.ds(pl.multiple_of(start, CHUNK), CHUNK)]
                dst = state.at[core, k, rows_here]
                if ds_ == 0 and dc == 0:
                    copy = pltpu.make_async_copy(src, dst, in_recv.at[0, 0, k])
                else:
                    copy = remote(src, dst, in_send.at[ds_, dc, k], in_recv.at[ds_, dc, k], rep_to, slab_to)
                copy.start()
                first_waits.append((k, copy))

    perms[me] = p_ref[0]

    def spread(k, carry):
        to = lax.rem(me + k, n_rep)
        remote(p_ref.at[0], perms.at[me], perm_send, perm_recv, to, slab).start()
        return carry

    lax.fori_loop(1, n_rep, spread, 0)
    others = perms.at[pl.ds(0, n_rep - 1)]
    spread_all = remote(others, others, perm_send, perm_recv, flipped(0), slab)

    def contribution(a, b):
        return lax.dot_general(a, b, (((1,), (1,)), ((), ())), preferred_element_type=jnp.float32)

    pending = []
    exchange = None
    for r in range(rounds):
        local_bit, device_bit, position = plan[r]
        last = r == rounds - 1

        mine = None if device_bit is None else bit(device_bit)
        stays = mine if last else bit(plan[r + 1][1])
        if r == 0:
            first, second = 1 - stays, stays
        else:
            same = 1 - (stays + mine) % 2 if not last else 1
            first, second = 2 * r + same, 2 * r + 1 - same
        base = 0
        for b, p in position.items():
            base = base + bit(p) * (1 << b)
        first_rep = base + (1 - stays) * (1 << local_bit)
        second_rep = base + stays * (1 << local_bit)

        partial = None
        for k in range(chunks):
            if r == 0:
                for at, copy in first_waits:
                    if at == k:
                        copy.wait()
            else:
                exchange[k].wait_recv()
            term = contribution(state[first, k], state[second, k])
            partial = term if partial is None else partial + term
        part[r] = partial.reshape(2, ffw // 2, ffw)
        to_core = remote(part.at[r, 1 - core], core_in.at[r], core_send.at[r], core_recv.at[r], flipped(0), slab)
        to_core.start()
        if r == 0:
            spread_all.wait()
        columns = lax.broadcasted_iota(jnp.int32, (ffw, ffw), 1)
        rows = lax.broadcasted_iota(jnp.int32, (ffw, ffw), 0)
        first_perm = perms[first_rep].astype(jnp.float32).T[:, r:r + 1].astype(jnp.int32)
        second_perm = perms[second_rep, r:r + 1, :]
        first_hot = (first_perm == columns).astype(jnp.float32)
        second_hot = (second_perm == rows).astype(jnp.float32)
        to_core.wait_recv()
        total = part[r, core] + core_in[r]
        slab_out[r] = total.astype(slab_out.dtype)
        to_slabs = []
        for ds_ in range(1, n_slab):
            copy = remote(slab_out.at[r], slab_in.at[r, ds_ - 1], slab_send.at[r, ds_ - 1],
                          slab_recv.at[r, ds_ - 1], me, (slab + ds_) % n_slab)
            copy.start()
            to_slabs.append(copy)
        for ds_ in range(1, n_slab):
            to_slabs[ds_ - 1].wait_recv()
            total = total + slab_in[r, ds_ - 1].astype(jnp.float32)
        cost_ref[r, core] = total
        to_cost = remote(cost_ref.at[r, core], cost_ref.at[r, core], cost_send.at[r], cost_recv.at[r],
                         flipped(0), slab)
        to_cost.start()
        to_cost.wait_recv()
        pending += [to_core, to_cost] + to_slabs

        cost = cost_ref[r].reshape(ffw, ffw) * (1.0 / math.sqrt(width))
        squared = cost * cost
        fourth = squared * squared
        by_row = 1.0 / (1.0 + jnp.sum(fourth, axis=1, keepdims=True))
        by_column = 1.0 / (1.0 + jnp.sum(fourth, axis=0, keepdims=True))
        first_mix = (first_hot + fourth * by_row).astype(jnp.bfloat16)
        second_mix = (second_hot + fourth * by_column).T.astype(jnp.bfloat16)

        def merged(own, mix, other):
            aligned = 0.5 * jnp.dot(mix, other, preferred_element_type=jnp.float32)
            return ((own.astype(jnp.float32) + aligned) * (1.0 / math.sqrt(2.0))).astype(jnp.bfloat16)

        if not last:
            to = flipped(plan[r + 1][1])
            exchange = []
            for k in range(chunks):
                sent[r, k] = merged(state[first, k], first_mix, state[second, k])
                copy = remote(sent.at[r, k], state.at[2 * (r + 1) + 1, k], ex_send.at[r, k], ex_recv.at[r, k], to, slab)
                copy.start()
                exchange.append(copy)
            for k in range(chunks):
                state[2 * (r + 1), k] = merged(state[second, k], second_mix, state[first, k])
            pending += exchange
        else:
            source = slab * 2 + core

            def deliver(buffer, at, owner, k):
                for h in range(n_slab):
                    column = source * block + k * CHUNK
                    src = buffer.at[k, pl.ds(h * half, half)]
                    dst = out_ref.at[0, :, pl.ds(pl.multiple_of(column, CHUNK), CHUNK)]
                    stay = jnp.logical_and(owner == me, slab == h)

                    @pl.when(stay)
                    def _():
                        pltpu.make_async_copy(src, dst, out_recv.at[source, k]).start()

                    @pl.when(jnp.logical_not(stay))
                    def _():
                        remote(src, dst, out_send.at[at, h, k], out_recv.at[source, k], owner, h).start()

            for k in range(chunks):
                sent[r, k] = merged(state[first, k], first_mix, state[second, k])
                deliver(sent.at[r], 0, first_rep, k)
                kept[k] = merged(state[second, k], second_mix, state[first, k])
                deliver(kept, 1, second_rep, k)
            for k in range(chunks):
                for s in range(2 * n_slab):
                    dst = out_ref.at[0, :, pl.ds(s * block + k * CHUNK, CHUNK)]
                    pltpu.make_async_copy(dst, dst, out_recv.at[s, k]).wait()
                for at, owner, buffer in ((0, first_rep, sent.at[r]), (1, second_rep, kept)):
                    for h in range(n_slab):
                        @pl.when(jnp.logical_not(jnp.logical_and(owner == me, slab == h)))
                        def _():
                            src = buffer.at[k, pl.ds(h * half, half)]
                            dst = out_ref.at[0, :, pl.ds(k * CHUNK, CHUNK)]
                            remote(src, dst, out_send.at[at, h, k], out_recv.at[0, k], owner, h).wait_send()
    for copy in pending:
        copy.wait_send()


def solution(mesh):
    n_rep, n_slab = mesh.shape["rep"], mesh.shape["slab"]

    def local(weights, perms):
        _, half, width = weights.shape
        rounds = perms.shape[1]
        ffw = perms.shape[2]
        chunks = width // (2 * n_slab) // CHUNK
        vmem = pltpu.VMEM
        dma = pltpu.SemaphoreType.DMA
        bf16, f32 = jnp.bfloat16, jnp.float32
        return pl.pallas_call(
            functools.partial(kernel, n_rep, n_slab, rounds),
            out_shape=jax.ShapeDtypeStruct(weights.shape, weights.dtype),
            in_specs=[pl.BlockSpec(memory_space=pltpu.VMEM)] * 2,
            out_specs=pl.BlockSpec(memory_space=pltpu.VMEM),
            scratch_shapes=[
                vmem((2 * rounds, chunks, ffw, CHUNK), bf16),
                vmem((rounds, chunks, ffw, CHUNK), bf16),
                vmem((chunks, ffw, CHUNK), bf16),
                vmem((rounds, 2, ffw // 2, ffw), f32),
                vmem((rounds, ffw // 2, ffw), f32),
                vmem((rounds, ffw // 2, ffw), bf16),
                vmem((rounds, n_slab - 1, ffw // 2, ffw), bf16),
                vmem((rounds, 2, ffw // 2, ffw), f32),
                vmem((n_rep, rounds, ffw), jnp.int32),
                dma((n_slab, 2, chunks)), dma((n_slab, 2, chunks)),
                dma((rounds, chunks)), dma((rounds, chunks)),
                dma((rounds,)), dma((rounds,)),
                dma((rounds, n_slab - 1)), dma((rounds, n_slab - 1)),
                dma((rounds,)), dma((rounds,)),
                dma((2, n_slab, chunks)), dma((2 * n_slab, chunks)),
                dma, dma,
            ],
            compiler_params=pltpu.CompilerParams(has_side_effects=True, vmem_limit_bytes=60 * 1024 * 1024),
        )(weights, perms)

    return jax.shard_map(
        local, mesh=mesh, in_specs=(P("rep", "slab", None), P("rep", None, None)),
        out_specs=P("rep", "slab", None), check_vma=False,
    )
```

```python
import functools
import math

import jax
import jax.numpy as jnp
from jax import lax
from jax.experimental import pallas as pl
from jax.experimental.pallas import tpu as pltpu
from jax.sharding import PartitionSpec as P

CHUNK = 256


def placements(bits, rounds):
    position = {b: b for b in range(1, bits)}
    plan = [(0, None, dict(position))]
    for r in range(1, rounds):
        old, new = (r - 1) % bits, r % bits
        device_bit = position.pop(new)
        position[old] = device_bit
        plan.append((new, device_bit, dict(position)))
    return plan


def kernel(n_rep, n_slab, rounds, w_ref, p_ref, out_ref,
           state, sent, kept, part, core_in, slab_out, slab_in, cost_ref, perms, hot,
           in_send, in_recv, ex_send, ex_recv, core_send, core_recv, slab_send, slab_recv,
           cost_send, cost_recv, out_send, out_recv, perm_send, perm_recv):
    bits = n_rep.bit_length() - 1
    me = lax.axis_index("rep")
    slab = lax.axis_index("slab")
    core = me % 2
    half, width = w_ref.shape[1], w_ref.shape[2]
    ffw = half * n_slab
    block = width // (2 * n_slab)
    chunks = block // CHUNK
    plan = placements(bits, rounds)

    def bit(b):
        return (me // (1 << b)) % 2

    def flipped(b):
        return me + (1 - 2 * bit(b)) * (1 << b)

    def remote(src, dst, send, recv, rep_to, slab_to):
        return pltpu.make_async_remote_copy(
            src_ref=src, dst_ref=dst, send_sem=send, recv_sem=recv,
            device_id=(rep_to, slab_to), device_id_type=pl.DeviceIdType.MESH)

    first_waits = []
    rows_here = pl.ds(pl.multiple_of(slab * half, half), half)
    for k in range(chunks):
        for ds_ in range(n_slab):
            for dc in range(2):
                rep_to = me if dc == 0 else flipped(0)
                core_to = core if dc == 0 else 1 - core
                slab_to = (slab + ds_) % n_slab
                start = (slab_to * 2 + core_to) * block + k * CHUNK
                src = w_ref.at[0, :, pl.ds(pl.multiple_of(start, CHUNK), CHUNK)]
                dst = state.at[core, k, rows_here]
                if ds_ == 0 and dc == 0:
                    copy = pltpu.make_async_copy(src, dst, in_recv.at[0, 0, k])
                else:
                    copy = remote(src, dst, in_send.at[ds_, dc, k], in_recv.at[ds_, dc, k], rep_to, slab_to)
                copy.start()
                first_waits.append((k, copy))

    perms[me] = p_ref[0]

    def spread(k, carry):
        to = lax.rem(me + k, n_rep)
        remote(p_ref.at[0], perms.at[me], perm_send, perm_recv, to, slab).start()
        return carry

    lax.fori_loop(1, n_rep, spread, 0)
    others = perms.at[pl.ds(0, n_rep - 1)]
    spread_all = remote(others, others, perm_send, perm_recv, flipped(0), slab)

    def contribution(a, b):
        return lax.dot_general(a, b, (((1,), (1,)), ((), ())), preferred_element_type=jnp.float32)

    pending = []
    exchange = None
    for r in range(rounds):
        local_bit, device_bit, position = plan[r]
        last = r == rounds - 1

        mine = None if device_bit is None else bit(device_bit)
        stays = mine if last else bit(plan[r + 1][1])
        if r == 0:
            first, second = 1 - stays, stays
        else:
            same = 1 - (stays + mine) % 2 if not last else 1
            first, second = 2 * r + same, 2 * r + 1 - same
        base = 0
        for b, p in position.items():
            base = base + bit(p) * (1 << b)
        first_rep = base + (1 - stays) * (1 << local_bit)
        second_rep = base + stays * (1 << local_bit)

        partial = None
        for k in range(chunks):
            if r == 0:
                for at, copy in first_waits:
                    if at == k:
                        copy.wait()
            else:
                exchange[0][k].wait_recv()
                exchange[1][k].wait_recv()
            term = contribution(state[first, k], state[second, k])
            partial = term if partial is None else partial + term
        part[r] = partial.reshape(2, ffw // 2, ffw)
        to_core = remote(part.at[r, 1 - core], core_in.at[r], core_send.at[r], core_recv.at[r], flipped(0), slab)
        to_core.start()
        if r == 0:
            spread_all.wait()
        columns = lax.broadcasted_iota(jnp.int32, (ffw, ffw), 1)
        rows = lax.broadcasted_iota(jnp.int32, (ffw, ffw), 0)
        first_perm = perms[first_rep].astype(jnp.float32).T[:, r:r + 1].astype(jnp.int32)
        second_perm = perms[second_rep, r:r + 1, :]
        first_hot = (first_perm == columns).astype(jnp.float32)
        second_hot = (second_perm == rows).astype(jnp.float32)
        to_core.wait_recv()
        total = part[r, core] + core_in[r]
        slab_out[r] = total.astype(slab_out.dtype)
        to_slabs = []
        for ds_ in range(1, n_slab):
            copy = remote(slab_out.at[r], slab_in.at[r, ds_ - 1], slab_send.at[r, ds_ - 1],
                          slab_recv.at[r, ds_ - 1], me, (slab + ds_) % n_slab)
            copy.start()
            to_slabs.append(copy)
        for ds_ in range(1, n_slab):
            to_slabs[ds_ - 1].wait_recv()
            total = total + slab_in[r, ds_ - 1].astype(jnp.float32)
        cost_ref[r, core] = total
        to_cost = remote(cost_ref.at[r, core], cost_ref.at[r, core], cost_send.at[r], cost_recv.at[r],
                         flipped(0), slab)
        to_cost.start()
        pending += [to_core, to_cost] + to_slabs

        scale = 1.0 / math.sqrt(width)
        mine_rows = pl.ds(pl.multiple_of(core * (ffw // 2), ffw // 2), ffw // 2)
        other_rows = pl.ds(pl.multiple_of((1 - core) * (ffw // 2), ffw // 2), ffw // 2)

        def merged(own, mix, other):
            aligned = 0.5 * jnp.dot(mix, other, preferred_element_type=jnp.float32)
            return ((own.astype(jnp.float32) + aligned) * (1.0 / math.sqrt(2.0))).astype(jnp.bfloat16)

        if last:
            source = slab * 2 + core

            def deliver(buffer, at, owner, h, k):
                column = source * block + k * CHUNK
                src = buffer.at[k, pl.ds(pl.multiple_of(h * half, half), half)]
                dst = out_ref.at[0, :, pl.ds(pl.multiple_of(column, CHUNK), CHUNK)]
                stay = jnp.logical_and(owner == me, slab == h)

                @pl.when(stay)
                def _():
                    pltpu.make_async_copy(src, dst, out_recv.at[source, k]).start()

                @pl.when(jnp.logical_not(stay))
                def _():
                    remote(src, dst, out_send.at[at, h, k], out_recv.at[source, k], owner, h).start()
        else:
            exchange = [[], []]

        fourths = []
        for part_at, its_rows in enumerate((mine_rows, other_rows)):
            if part_at == 1:
                to_cost.wait_recv()
            cost = (total if part_at == 0 else cost_ref[r, 1 - core]) * scale
            squared = cost * cost
            fourth = squared * squared
            fourths.append(fourth)
            by_row = 1.0 / (1.0 + jnp.sum(fourth, axis=1, keepdims=True))
            if part_at == 0:
                hot[...] = first_hot
            mix = (hot[its_rows, :] + fourth * by_row).astype(jnp.bfloat16)
            for k in range(chunks):
                sent[r, k, its_rows, :] = merged(state[first, k, its_rows, :], mix, state[second, k])
                if not last:
                    copy = remote(sent.at[r, k, its_rows], state.at[2 * (r + 1) + 1, k, its_rows],
                                  ex_send.at[r, part_at, k], ex_recv.at[r, part_at, k],
                                  flipped(plan[r + 1][1]), slab)
                    copy.start()
                    exchange[part_at].append(copy)
                elif n_slab == 2:
                    deliver(sent.at[r], 0, first_rep, core if part_at == 0 else 1 - core, k)
            if last and n_slab != 2 and part_at == 1:
                for k in range(chunks):
                    for h in range(n_slab):
                        deliver(sent.at[r], 0, first_rep, h, k)
        by_column = 1.0 / (1.0 + sum(jnp.sum(f, axis=0, keepdims=True) for f in fourths))
        for f, its_rows in zip(fourths, (mine_rows, other_rows)):
            hot[its_rows, :] = f * by_column
        second_mix = (second_hot + hot[...]).T.astype(jnp.bfloat16)
        for k in range(chunks):
            new = merged(state[second, k], second_mix, state[first, k])
            if last:
                kept[k] = new
                for h in range(n_slab):
                    deliver(kept, 1, second_rep, h, k)
            else:
                state[2 * (r + 1), k] = new
        if not last:
            pending += exchange[0] + exchange[1]
        else:
            for k in range(chunks):
                for s in range(2 * n_slab):
                    dst = out_ref.at[0, :, pl.ds(s * block + k * CHUNK, CHUNK)]
                    pltpu.make_async_copy(dst, dst, out_recv.at[s, k]).wait()
                for at, owner, buffer in ((0, first_rep, sent.at[r]), (1, second_rep, kept)):
                    for h in range(n_slab):
                        @pl.when(jnp.logical_not(jnp.logical_and(owner == me, slab == h)))
                        def _():
                            src = buffer.at[k, pl.ds(h * half, half)]
                            dst = out_ref.at[0, :, pl.ds(k * CHUNK, CHUNK)]
                            remote(src, dst, out_send.at[at, h, k], out_recv.at[0, k], owner, h).wait_send()
    for copy in pending:
        copy.wait_send()


def solution(mesh):
    n_rep, n_slab = mesh.shape["rep"], mesh.shape["slab"]

    def local(weights, perms):
        _, half, width = weights.shape
        rounds = perms.shape[1]
        ffw = perms.shape[2]
        chunks = width // (2 * n_slab) // CHUNK
        vmem = pltpu.VMEM
        dma = pltpu.SemaphoreType.DMA
        bf16, f32 = jnp.bfloat16, jnp.float32
        return pl.pallas_call(
            functools.partial(kernel, n_rep, n_slab, rounds),
            out_shape=jax.ShapeDtypeStruct(weights.shape, weights.dtype),
            in_specs=[pl.BlockSpec(memory_space=pltpu.VMEM)] * 2,
            out_specs=pl.BlockSpec(memory_space=pltpu.VMEM),
            scratch_shapes=[
                vmem((2 * rounds, chunks, ffw, CHUNK), bf16),
                vmem((rounds, chunks, ffw, CHUNK), bf16),
                vmem((chunks, ffw, CHUNK), bf16),
                vmem((rounds, 2, ffw // 2, ffw), f32),
                vmem((rounds, ffw // 2, ffw), f32),
                vmem((rounds, ffw // 2, ffw), bf16),
                vmem((rounds, n_slab - 1, ffw // 2, ffw), bf16),
                vmem((rounds, 2, ffw // 2, ffw), f32),
                vmem((n_rep, rounds, ffw), jnp.int32),
                vmem((ffw, ffw), f32),
                dma((n_slab, 2, chunks)), dma((n_slab, 2, chunks)),
                dma((rounds, 2, chunks)), dma((rounds, 2, chunks)),
                dma((rounds,)), dma((rounds,)),
                dma((rounds, n_slab - 1)), dma((rounds, n_slab - 1)),
                dma((rounds,)), dma((rounds,)),
                dma((2, n_slab, chunks)), dma((2 * n_slab, chunks)),
                dma, dma,
            ],
            compiler_params=pltpu.CompilerParams(has_side_effects=True, vmem_limit_bytes=60 * 1024 * 1024),
        )(weights, perms)

    return jax.shard_map(
        local, mesh=mesh, in_specs=(P("rep", "slab", None), P("rep", None, None)),
        out_specs=P("rep", "slab", None), check_vma=False,
    )
```

```python
import functools
import math

import jax
import jax.numpy as jnp
from jax import lax
from jax.experimental import pallas as pl
from jax.experimental.pallas import tpu as pltpu
from jax.sharding import PartitionSpec as P

CHUNK = 256


def placements(bits, rounds):
    position = {b: b for b in range(1, bits)}
    plan = [(0, None, dict(position))]
    for r in range(1, rounds):
        old, new = (r - 1) % bits, r % bits
        device_bit = position.pop(new)
        position[old] = device_bit
        plan.append((new, device_bit, dict(position)))
    return plan


def kernel(n_rep, n_slab, rounds, w_ref, p_ref, out_ref,
           state, sent, kept, part, core_in, slab_out, slab_in, cost_ref, perms, hot,
           in_send, in_recv, ex_send, ex_recv, core_send, core_recv, slab_send, slab_recv,
           cost_send, cost_recv, out_send, out_recv, perm_send, perm_recv):
    bits = n_rep.bit_length() - 1
    me = lax.axis_index("rep")
    slab = lax.axis_index("slab")
    core = me % 2
    half, width = w_ref.shape[1], w_ref.shape[2]
    ffw = half * n_slab
    block = width // (2 * n_slab)
    chunks = block // CHUNK
    plan = placements(bits, rounds)

    def bit(b):
        return (me // (1 << b)) % 2

    def flipped(b):
        return me + (1 - 2 * bit(b)) * (1 << b)

    def remote(src, dst, send, recv, rep_to, slab_to):
        return pltpu.make_async_remote_copy(
            src_ref=src, dst_ref=dst, send_sem=send, recv_sem=recv,
            device_id=(rep_to, slab_to), device_id_type=pl.DeviceIdType.MESH)

    barrier = pltpu.get_barrier_semaphore()
    devices = n_rep * n_slab

    def greet(k, carry):
        to = lax.rem(me * n_slab + slab + k, devices)
        pl.semaphore_signal(barrier, inc=1, device_id=(to // n_slab, to % n_slab),
                            device_id_type=pl.DeviceIdType.MESH)
        return carry

    lax.fori_loop(1, devices, greet, 0)
    pl.semaphore_wait(barrier, devices - 1)

    first_waits = []
    rows_here = pl.ds(pl.multiple_of(slab * half, half), half)
    for k in range(chunks):
        for ds_ in range(n_slab):
            for dc in range(2):
                rep_to = me if dc == 0 else flipped(0)
                core_to = core if dc == 0 else 1 - core
                slab_to = (slab + ds_) % n_slab
                start = (slab_to * 2 + core_to) * block + k * CHUNK
                src = w_ref.at[0, :, pl.ds(pl.multiple_of(start, CHUNK), CHUNK)]
                dst = state.at[core, k, rows_here]
                if ds_ == 0 and dc == 0:
                    copy = pltpu.make_async_copy(src, dst, in_recv.at[0, 0, k])
                else:
                    copy = remote(src, dst, in_send.at[ds_, dc, k], in_recv.at[ds_, dc, k], rep_to, slab_to)
                copy.start()
                first_waits.append((k, copy))

    perms[me] = p_ref[0]

    def spread(k, carry):
        to = lax.rem(me + k, n_rep)
        remote(p_ref.at[0], perms.at[me], perm_send, perm_recv, to, slab).start()
        return carry

    lax.fori_loop(1, n_rep, spread, 0)
    others = perms.at[pl.ds(0, n_rep - 1)]
    spread_all = remote(others, others, perm_send, perm_recv, flipped(0), slab)

    def contribution(a, b):
        return lax.dot_general(a, b, (((1,), (1,)), ((), ())), preferred_element_type=jnp.float32)

    pending = []
    exchange = None
    for r in range(rounds):
        local_bit, device_bit, position = plan[r]
        last = r == rounds - 1

        mine = None if device_bit is None else bit(device_bit)
        stays = mine if last else bit(plan[r + 1][1])
        if r == 0:
            first, second = 1 - stays, stays
        else:
            same = 1 - (stays + mine) % 2 if not last else 1
            first, second = 2 * r + same, 2 * r + 1 - same
        base = 0
        for b, p in position.items():
            base = base + bit(p) * (1 << b)
        first_rep = base + (1 - stays) * (1 << local_bit)
        second_rep = base + stays * (1 << local_bit)

        partial = None
        for k in range(chunks):
            if r == 0:
                for at, copy in first_waits:
                    if at == k:
                        copy.wait()
            else:
                exchange[0][k].wait_recv()
                exchange[1][k].wait_recv()
            term = contribution(state[first, k], state[second, k])
            partial = term if partial is None else partial + term
        part[r] = partial.reshape(2, ffw // 2, ffw)
        to_core = remote(part.at[r, 1 - core], core_in.at[r], core_send.at[r], core_recv.at[r], flipped(0), slab)
        to_core.start()
        if r == 0:
            spread_all.wait()
        columns = lax.broadcasted_iota(jnp.int32, (ffw, ffw), 1)
        rows = lax.broadcasted_iota(jnp.int32, (ffw, ffw), 0)
        first_perm = perms[first_rep].astype(jnp.float32).T[:, r:r + 1].astype(jnp.int32)
        second_perm = perms[second_rep, r:r + 1, :]
        first_hot = (first_perm == columns).astype(jnp.float32)
        second_hot = (second_perm == rows).astype(jnp.float32)
        to_core.wait_recv()
        total = part[r, core] + core_in[r]
        slab_out[r] = total.astype(slab_out.dtype)
        to_slabs = []
        for ds_ in range(1, n_slab):
            copy = remote(slab_out.at[r], slab_in.at[r, ds_ - 1], slab_send.at[r, ds_ - 1],
                          slab_recv.at[r, ds_ - 1], me, (slab + ds_) % n_slab)
            copy.start()
            to_slabs.append(copy)
        for ds_ in range(1, n_slab):
            to_slabs[ds_ - 1].wait_recv()
            total = total + slab_in[r, ds_ - 1].astype(jnp.float32)
        cost_ref[r, core] = total
        to_cost = remote(cost_ref.at[r, core], cost_ref.at[r, core], cost_send.at[r], cost_recv.at[r],
                         flipped(0), slab)
        to_cost.start()
        pending += [to_core, to_cost] + to_slabs

        scale = 1.0 / math.sqrt(width)
        mine_rows = pl.ds(pl.multiple_of(core * (ffw // 2), ffw // 2), ffw // 2)
        other_rows = pl.ds(pl.multiple_of((1 - core) * (ffw // 2), ffw // 2), ffw // 2)

        def merged(own, mix, other):
            aligned = 0.5 * jnp.dot(mix, other, preferred_element_type=jnp.float32)
            return ((own.astype(jnp.float32) + aligned) * (1.0 / math.sqrt(2.0))).astype(jnp.bfloat16)

        if last:
            source = slab * 2 + core

            def deliver(buffer, at, owner, h, k):
                column = source * block + k * CHUNK
                src = buffer.at[k, pl.ds(pl.multiple_of(h * half, half), half)]
                dst = out_ref.at[0, :, pl.ds(pl.multiple_of(column, CHUNK), CHUNK)]
                stay = jnp.logical_and(owner == me, slab == h)

                @pl.when(stay)
                def _():
                    pltpu.make_async_copy(src, dst, out_recv.at[source, k]).start()

                @pl.when(jnp.logical_not(stay))
                def _():
                    remote(src, dst, out_send.at[at, h, k], out_recv.at[source, k], owner, h).start()
        else:
            exchange = [[], []]

        fourths = []
        for part_at, its_rows in enumerate((mine_rows, other_rows)):
            if part_at == 1:
                to_cost.wait_recv()
            cost = (total if part_at == 0 else cost_ref[r, 1 - core]) * scale
            squared = cost * cost
            fourth = squared * squared
            fourths.append(fourth)
            by_row = 1.0 / (1.0 + jnp.sum(fourth, axis=1, keepdims=True))
            if part_at == 0:
                hot[...] = first_hot
            mix = (hot[its_rows, :] + fourth * by_row).astype(jnp.bfloat16)
            for k in range(chunks):
                sent[r, k, its_rows, :] = merged(state[first, k, its_rows, :], mix, state[second, k])
                if not last:
                    copy = remote(sent.at[r, k, its_rows], state.at[2 * (r + 1) + 1, k, its_rows],
                                  ex_send.at[r, part_at, k], ex_recv.at[r, part_at, k],
                                  flipped(plan[r + 1][1]), slab)
                    copy.start()
                    exchange[part_at].append(copy)
                elif n_slab == 2:
                    deliver(sent.at[r], 0, first_rep, core if part_at == 0 else 1 - core, k)
            if last and n_slab != 2 and part_at == 1:
                for k in range(chunks):
                    for h in range(n_slab):
                        deliver(sent.at[r], 0, first_rep, h, k)
        by_column = 1.0 / (1.0 + sum(jnp.sum(f, axis=0, keepdims=True) for f in fourths))
        for f, its_rows in zip(fourths, (mine_rows, other_rows)):
            hot[its_rows, :] = f * by_column
        second_mix = (second_hot + hot[...]).T.astype(jnp.bfloat16)
        for k in range(chunks):
            new = merged(state[second, k], second_mix, state[first, k])
            if last:
                kept[k] = new
                for h in range(n_slab):
                    deliver(kept, 1, second_rep, h, k)
            else:
                state[2 * (r + 1), k] = new
        if not last:
            pending += exchange[0] + exchange[1]
        else:
            for k in range(chunks):
                for s in range(2 * n_slab):
                    dst = out_ref.at[0, :, pl.ds(s * block + k * CHUNK, CHUNK)]
                    pltpu.make_async_copy(dst, dst, out_recv.at[s, k]).wait()
                for at, owner, buffer in ((0, first_rep, sent.at[r]), (1, second_rep, kept)):
                    for h in range(n_slab):
                        @pl.when(jnp.logical_not(jnp.logical_and(owner == me, slab == h)))
                        def _():
                            src = buffer.at[k, pl.ds(h * half, half)]
                            dst = out_ref.at[0, :, pl.ds(k * CHUNK, CHUNK)]
                            remote(src, dst, out_send.at[at, h, k], out_recv.at[0, k], owner, h).wait_send()
    for copy in pending:
        copy.wait_send()


def solution(mesh):
    n_rep, n_slab = mesh.shape["rep"], mesh.shape["slab"]

    def local(weights, perms):
        _, half, width = weights.shape
        rounds = perms.shape[1]
        ffw = perms.shape[2]
        chunks = width // (2 * n_slab) // CHUNK
        vmem = pltpu.VMEM
        dma = pltpu.SemaphoreType.DMA
        bf16, f32 = jnp.bfloat16, jnp.float32
        return pl.pallas_call(
            functools.partial(kernel, n_rep, n_slab, rounds),
            out_shape=jax.ShapeDtypeStruct(weights.shape, weights.dtype),
            in_specs=[pl.BlockSpec(memory_space=pltpu.VMEM)] * 2,
            out_specs=pl.BlockSpec(memory_space=pltpu.VMEM),
            scratch_shapes=[
                vmem((2 * rounds, chunks, ffw, CHUNK), bf16),
                vmem((rounds, chunks, ffw, CHUNK), bf16),
                vmem((chunks, ffw, CHUNK), bf16),
                vmem((rounds, 2, ffw // 2, ffw), f32),
                vmem((rounds, ffw // 2, ffw), f32),
                vmem((rounds, ffw // 2, ffw), bf16),
                vmem((rounds, n_slab - 1, ffw // 2, ffw), bf16),
                vmem((rounds, 2, ffw // 2, ffw), f32),
                vmem((n_rep, rounds, ffw), jnp.int32),
                vmem((ffw, ffw), f32),
                dma((n_slab, 2, chunks)), dma((n_slab, 2, chunks)),
                dma((rounds, 2, chunks)), dma((rounds, 2, chunks)),
                dma((rounds,)), dma((rounds,)),
                dma((rounds, n_slab - 1)), dma((rounds, n_slab - 1)),
                dma((rounds,)), dma((rounds,)),
                dma((2, n_slab, chunks)), dma((2 * n_slab, chunks)),
                dma, dma,
            ],
            compiler_params=pltpu.CompilerParams(collective_id=0, has_side_effects=True, vmem_limit_bytes=60 * 1024 * 1024),
        )(weights, perms)

    return jax.shard_map(
        local, mesh=mesh, in_specs=(P("rep", "slab", None), P("rep", None, None)),
        out_specs=P("rep", "slab", None), check_vma=False,
    )
```

```python
import functools
import math

import jax
import jax.numpy as jnp
from jax import lax
from jax.experimental import pallas as pl
from jax.experimental.pallas import tpu as pltpu
from jax.sharding import PartitionSpec as P

CHUNK = 256
PIECES = 2


def placements(bits, rounds):
    position = {b: b for b in range(1, bits)}
    plan = [(0, None, dict(position))]
    for r in range(1, rounds):
        old, new = (r - 1) % bits, r % bits
        device_bit = position.pop(new)
        position[old] = device_bit
        plan.append((new, device_bit, dict(position)))
    return plan


def kernel(n_rep, n_slab, rounds, w_ref, p_ref, out_ref,
           state, sent, kept, part, core_in, slab_out, slab_in, cost_ref, perms, hot,
           in_send, in_recv, ex_send, ex_recv, core_send, core_recv, slab_send, slab_recv,
           cost_send, cost_recv, out_send, out_recv, perm_send, perm_recv):
    bits = n_rep.bit_length() - 1
    me = lax.axis_index("rep")
    slab = lax.axis_index("slab")
    core = me % 2
    half, width = w_ref.shape[1], w_ref.shape[2]
    ffw = half * n_slab
    block = width // (2 * n_slab)
    chunks = block // CHUNK
    plan = placements(bits, rounds)

    def bit(b):
        return (me // (1 << b)) % 2

    def flipped(b):
        return me + (1 - 2 * bit(b)) * (1 << b)

    def remote(src, dst, send, recv, rep_to, slab_to):
        return pltpu.make_async_remote_copy(
            src_ref=src, dst_ref=dst, send_sem=send, recv_sem=recv,
            device_id=(rep_to, slab_to), device_id_type=pl.DeviceIdType.MESH)

    barrier = pltpu.get_barrier_semaphore()
    devices = n_rep * n_slab

    def greet(k, carry):
        to = lax.rem(me * n_slab + slab + k, devices)
        pl.semaphore_signal(barrier, inc=1, device_id=(to // n_slab, to % n_slab),
                            device_id_type=pl.DeviceIdType.MESH)
        return carry

    lax.fori_loop(1, devices, greet, 0)
    pl.semaphore_wait(barrier, devices - 1)

    first_waits = []
    rows_here = pl.ds(pl.multiple_of(slab * half, half), half)
    for k in range(chunks):
        for ds_ in range(n_slab):
            for dc in range(2):
                rep_to = me if dc == 0 else flipped(0)
                core_to = core if dc == 0 else 1 - core
                slab_to = (slab + ds_) % n_slab
                start = (slab_to * 2 + core_to) * block + k * CHUNK
                src = w_ref.at[0, :, pl.ds(pl.multiple_of(start, CHUNK), CHUNK)]
                dst = state.at[core, k, rows_here]
                if ds_ == 0 and dc == 0:
                    copy = pltpu.make_async_copy(src, dst, in_recv.at[0, 0, k])
                else:
                    copy = remote(src, dst, in_send.at[ds_, dc, k], in_recv.at[ds_, dc, k], rep_to, slab_to)
                copy.start()
                first_waits.append((k, copy))

    perms[me] = p_ref[0]

    def spread(k, carry):
        to = lax.rem(me + k, n_rep)
        remote(p_ref.at[0], perms.at[me], perm_send, perm_recv, to, slab).start()
        return carry

    lax.fori_loop(1, n_rep, spread, 0)
    others = perms.at[pl.ds(0, n_rep - 1)]
    spread_all = remote(others, others, perm_send, perm_recv, flipped(0), slab)

    def contribution(a, b):
        return lax.dot_general(a, b, (((1,), (1,)), ((), ())), preferred_element_type=jnp.float32)

    pending = []
    exchange = None
    for r in range(rounds):
        local_bit, device_bit, position = plan[r]
        last = r == rounds - 1

        mine = None if device_bit is None else bit(device_bit)
        stays = mine if last else bit(plan[r + 1][1])
        if r == 0:
            first, second = 1 - stays, stays
        else:
            same = 1 - (stays + mine) % 2 if not last else 1
            first, second = 2 * r + same, 2 * r + 1 - same
        base = 0
        for b, p in position.items():
            base = base + bit(p) * (1 << b)
        first_rep = base + (1 - stays) * (1 << local_bit)
        second_rep = base + stays * (1 << local_bit)

        partial = None
        for k in range(chunks):
            if r == 0:
                for at, copy in first_waits:
                    if at == k:
                        copy.wait()
            else:
                for piece in exchange:
                    piece[k].wait_recv()
            term = contribution(state[first, k], state[second, k])
            partial = term if partial is None else partial + term
        part[r] = partial.reshape(2, ffw // 2, ffw)
        quarter = ffw // 2 // PIECES
        to_cores = []
        for q in range(PIECES):
            its = pl.ds(q * quarter, quarter)
            copy = remote(part.at[r, 1 - core, its], core_in.at[r, its], core_send.at[r, q], core_recv.at[r, q],
                          flipped(0), slab)
            copy.start()
            to_cores.append(copy)
        if r == 0:
            spread_all.wait()
        columns = lax.broadcasted_iota(jnp.int32, (ffw, ffw), 1)
        rows = lax.broadcasted_iota(jnp.int32, (ffw, ffw), 0)
        first_perm = perms[first_rep].astype(jnp.float32).T[:, r:r + 1].astype(jnp.int32)
        second_perm = perms[second_rep, r:r + 1, :]
        first_hot = (first_perm == columns).astype(jnp.float32)
        second_hot = (second_perm == rows).astype(jnp.float32)
        to_slabs = []
        for q in range(PIECES):
            its = pl.ds(q * quarter, quarter)
            to_cores[q].wait_recv()
            total = part[r, core, its, :] + core_in[r, its, :]
            cost_ref[r, core, its, :] = total
            slab_out[r, its, :] = total.astype(slab_out.dtype)
            for ds_ in range(1, n_slab):
                copy = remote(slab_out.at[r, its], slab_in.at[r, ds_ - 1, its], slab_send.at[r, ds_ - 1, q],
                              slab_recv.at[r, ds_ - 1, q], me, (slab + ds_) % n_slab)
                copy.start()
                to_slabs.append(copy)
        to_costs = []
        pending += to_cores + to_slabs

        scale = 1.0 / math.sqrt(width)
        half_rows = ffw // 2
        row_sets = [pl.ds(pl.multiple_of(core * half_rows + q * quarter, quarter), quarter) for q in range(PIECES)]
        row_sets += [pl.ds(pl.multiple_of((1 - core) * half_rows + q * quarter, quarter), quarter)
                     for q in range(PIECES)]

        def merged(own, mix, other):
            aligned = 0.5 * jnp.dot(mix, other, preferred_element_type=jnp.float32)
            return ((own.astype(jnp.float32) + aligned) * (1.0 / math.sqrt(2.0))).astype(jnp.bfloat16)

        if last:
            source = slab * 2 + core

            def deliver(buffer, at, owner, h, k):
                column = source * block + k * CHUNK
                src = buffer.at[k, pl.ds(pl.multiple_of(h * half, half), half)]
                dst = out_ref.at[0, :, pl.ds(pl.multiple_of(column, CHUNK), CHUNK)]
                stay = jnp.logical_and(owner == me, slab == h)

                @pl.when(stay)
                def _():
                    pltpu.make_async_copy(src, dst, out_recv.at[source, k]).start()

                @pl.when(jnp.logical_not(stay))
                def _():
                    remote(src, dst, out_send.at[at, h, k], out_recv.at[source, k], owner, h).start()
        else:
            exchange = [[] for _ in row_sets]

        fourths = []
        for part_at, its_rows in enumerate(row_sets):
            q = part_at % PIECES
            its = pl.ds(q * quarter, quarter)
            if part_at < PIECES:
                total = cost_ref[r, core, its, :]
                for ds_ in range(1, n_slab):
                    to_slabs[q * (n_slab - 1) + ds_ - 1].wait_recv()
                    total = total + slab_in[r, ds_ - 1, its, :].astype(jnp.float32)
                cost_ref[r, core, its, :] = total
                copy = remote(cost_ref.at[r, core, its], cost_ref.at[r, core, its], cost_send.at[r, q],
                              cost_recv.at[r, q], flipped(0), slab)
                copy.start()
                to_costs.append(copy)
            else:
                to_costs[q].wait_recv()
                total = cost_ref[r, 1 - core, its, :]
            cost = total * scale
            squared = cost * cost
            fourth = squared * squared
            fourths.append(fourth)
            by_row = 1.0 / (1.0 + jnp.sum(fourth, axis=1, keepdims=True))
            if part_at == 0:
                hot[...] = first_hot
            mix = (hot[its_rows, :] + fourth * by_row).astype(jnp.bfloat16)
            for k in range(chunks):
                sent[r, k, its_rows, :] = merged(state[first, k, its_rows, :], mix, state[second, k])
                if not last:
                    copy = remote(sent.at[r, k, its_rows], state.at[2 * (r + 1) + 1, k, its_rows],
                                  ex_send.at[r, part_at, k], ex_recv.at[r, part_at, k],
                                  flipped(plan[r + 1][1]), slab)
                    copy.start()
                    exchange[part_at].append(copy)
                elif n_slab == 2 and q == PIECES - 1:
                    deliver(sent.at[r], 0, first_rep, core if part_at < PIECES else 1 - core, k)
            if last and n_slab != 2 and part_at == len(row_sets) - 1:
                for k in range(chunks):
                    for h in range(n_slab):
                        deliver(sent.at[r], 0, first_rep, h, k)
        by_column = 1.0 / (1.0 + sum(jnp.sum(f, axis=0, keepdims=True) for f in fourths))
        for f, its_rows in zip(fourths, row_sets):
            hot[its_rows, :] = f * by_column
        second_mix = (second_hot + hot[...]).T.astype(jnp.bfloat16)
        for k in range(chunks):
            new = merged(state[second, k], second_mix, state[first, k])
            if last:
                kept[k] = new
                for h in range(n_slab):
                    deliver(kept, 1, second_rep, h, k)
            else:
                state[2 * (r + 1), k] = new
        if not last:
            pending += sum(exchange, []) + to_costs
        else:
            pending += to_costs
            for k in range(chunks):
                for s in range(2 * n_slab):
                    dst = out_ref.at[0, :, pl.ds(s * block + k * CHUNK, CHUNK)]
                    pltpu.make_async_copy(dst, dst, out_recv.at[s, k]).wait()
                for at, owner, buffer in ((0, first_rep, sent.at[r]), (1, second_rep, kept)):
                    for h in range(n_slab):
                        @pl.when(jnp.logical_not(jnp.logical_and(owner == me, slab == h)))
                        def _():
                            src = buffer.at[k, pl.ds(h * half, half)]
                            dst = out_ref.at[0, :, pl.ds(k * CHUNK, CHUNK)]
                            remote(src, dst, out_send.at[at, h, k], out_recv.at[0, k], owner, h).wait_send()
    for copy in pending:
        copy.wait_send()


def solution(mesh):
    n_rep, n_slab = mesh.shape["rep"], mesh.shape["slab"]

    def local(weights, perms):
        _, half, width = weights.shape
        rounds = perms.shape[1]
        ffw = perms.shape[2]
        chunks = width // (2 * n_slab) // CHUNK
        vmem = pltpu.VMEM
        dma = pltpu.SemaphoreType.DMA
        bf16, f32 = jnp.bfloat16, jnp.float32
        return pl.pallas_call(
            functools.partial(kernel, n_rep, n_slab, rounds),
            out_shape=jax.ShapeDtypeStruct(weights.shape, weights.dtype),
            in_specs=[pl.BlockSpec(memory_space=pltpu.VMEM)] * 2,
            out_specs=pl.BlockSpec(memory_space=pltpu.VMEM),
            scratch_shapes=[
                vmem((2 * rounds, chunks, ffw, CHUNK), bf16),
                vmem((rounds, chunks, ffw, CHUNK), bf16),
                vmem((chunks, ffw, CHUNK), bf16),
                vmem((rounds, 2, ffw // 2, ffw), f32),
                vmem((rounds, ffw // 2, ffw), f32),
                vmem((rounds, ffw // 2, ffw), bf16),
                vmem((rounds, n_slab - 1, ffw // 2, ffw), bf16),
                vmem((rounds, 2, ffw // 2, ffw), f32),
                vmem((n_rep, rounds, ffw), jnp.int32),
                vmem((ffw, ffw), f32),
                dma((n_slab, 2, chunks)), dma((n_slab, 2, chunks)),
                dma((rounds, 2 * PIECES, chunks)), dma((rounds, 2 * PIECES, chunks)),
                dma((rounds, PIECES)), dma((rounds, PIECES)),
                dma((rounds, n_slab - 1, PIECES)), dma((rounds, n_slab - 1, PIECES)),
                dma((rounds, PIECES)), dma((rounds, PIECES)),
                dma((2, n_slab, chunks)), dma((2 * n_slab, chunks)),
                dma, dma,
            ],
            compiler_params=pltpu.CompilerParams(collective_id=0, has_side_effects=True, vmem_limit_bytes=60 * 1024 * 1024),
        )(weights, perms)

    return jax.shard_map(
        local, mesh=mesh, in_specs=(P("rep", "slab", None), P("rep", None, None)),
        out_specs=P("rep", "slab", None), check_vma=False,
    )
```
